256 devices in a mesh: rows: 64 (over x, z_hi, y, core), feat: 4 (over z_lo).
Axes of the slice: x: 4, y: 4, z: 8 (z_hi: 2, z_lo: 4; z = z_hi * 4 + z_lo), core: 2. Of those that a mesh axis runs over, the one named last changes fastest.
Arguments:
- bins: int32 [65536, 512], P('rows', 'feat'), may hold values from -2147483648 to 2147483647, as said below
- hessian: float32 [262144], P('rows'), may hold values from 0.05 to 1
- thresholds: float32 [128], replicated, may hold values from 0.02 to 0.98
Outputs:
- cuts: float32 [512, 128], P('feat')
The draws below stay inside these ranges and needn't reach their ends.
Inputs may be any that keep to these rules, and one draw needn't show every extreme that they name: `bins`: each word holds the bin ids, 0 to 255, of rows 4i to 4i + 3 of one feature, row 4i + k in bits 8k to 8k + 7 of the two's complement word.
All inputs are finite; a program needn't handle non-finite values.
Results may differ from the reference program's by a relative error of at most 0.000065.
Values sent between devices are 32-bit elements; how exact they have to be, the bound alone decides.
No kernel may reach another device: no remote copies, remote signals or barrier semaphores. Data moves between devices by JAX's collectives and lax.ppermute only.
A program may use at most 192 MiB of HBM per device.

```python
import math
import jax
import jax.numpy as jnp

F = 512
BINS = 256
Q = 128
ROW_DEV = 4096
ROWS = 262144
N_ROWS = 64


def draw_bins(key, part):
    key = jax.random.fold_in(key, 17)
    first, second, third, fourth = jax.random.split(key, 4)
    spread = jax.random.randint(first, (ROWS, F), 0, BINS)
    centers = jax.random.randint(second, (N_ROWS, F), 0, BINS)
    offsets = jax.random.randint(third, (ROWS, F), 0, 8)
    banded = jax.random.randint(fourth, (ROWS, F), 0, 2) == 0
    owner = jnp.arange(ROWS, dtype=jnp.int32) // ROW_DEV
    center_rows = centers[owner]
    ids = jnp.where(banded, (center_rows + offsets) % BINS, spread).astype(jnp.int32)
    grouped = ids.reshape(ROWS // 4, 4, F)
    packed = jnp.zeros((ROWS // 4, F), jnp.int32)
    for k in range(4):
        packed = jnp.bitwise_or(packed, jnp.left_shift(grouped[:, k, :], 8 * k))
    return packed.astype(jnp.int32)


def block_levels(own_key, dims, pieces, least, largest):
    loudness = 1.0
    for dim, shards_of in pieces:
        heights = jax.random.uniform(jax.random.fold_in(jax.random.fold_in(own_key, 6), dim), (shards_of,), jnp.float32, least / len(pieces), largest / len(pieces))
        loudness = loudness * jnp.repeat(jnp.exp(heights), dims[dim] // shards_of).reshape((-1,) + (1,) * (len(dims) - 1 - dim))
    return loudness


def setup_inputs(seed: int = 0) -> dict:
    key_list = jax.random.split(jax.random.key(seed), 4)
    return {
        "bins": draw_bins(jax.random.fold_in(key_list[3], 71), 0),
        "hessian": jnp.clip(jnp.exp(math.log(1.0) - 2.9957323 * jax.random.uniform(key_list[1], (ROWS,), jnp.float32) ** block_levels(key_list[1], (ROWS,), ((0, 64),), -0.2, 0.2)), 0.05, 1.0),
        "thresholds": jnp.clip(jax.random.uniform(key_list[2], (Q,), jnp.float32, 0.02, 0.98), 0.02, 0.98),
    }


def unpack(words):
    parts = [jnp.bitwise_and(jnp.right_shift(words, 8 * k), 255) for k in range(4)]
    stacked = jnp.stack(parts, axis=1)
    return stacked.reshape(words.shape[0] * 4, words.shape[1]).astype(jnp.int32)


def cut_positions(hist, thresholds):
    cum = jnp.cumsum(hist, axis=1)
    before = cum - hist
    total = cum[:, -1]
    target = thresholds[None, :, None] * total[:, None, None]
    ratio = (target - before[:, None, :]) / (hist[:, None, :] + 1.0)
    return jnp.sum(jnp.clip(ratio, 0.0, 1.0), axis=2)


def reference(bins, hessian, thresholds):
    ids = unpack(bins)

    def one_feature(column):
        return jax.ops.segment_sum(hessian, column, num_segments=BINS)

    hist = jax.vmap(one_feature)(ids.T).astype(jnp.float32)
    return cut_positions(hist, thresholds)
```

```python
import jax
import jax.numpy as jnp
from jax import lax
from jax.experimental import pallas as pl
from jax.experimental.pallas import tpu as pltpu
from jax.sharding import Mesh
from jax.sharding import PartitionSpec as P

BINS = 256
HI = 8
LO = 32
GROUP = 8
TERMS = 2


def hist_kernel(bins_ref, hess_ref, out_ref, words_ref, wts_ref):
    words, width = bins_ref.shape
    for i in range(words // 128):
        words_ref[:, pl.ds(128 * i, 128)] = bins_ref[pl.ds(128 * i, 128), :].T
    rest = hess_ref[...]
    for t in range(TERMS):
        part = rest.astype(jnp.bfloat16)
        rest = rest - part.astype(jnp.float32)
        for k in range(4):
            wts_ref[t, k] = jnp.broadcast_to(part[k : k + 1, :], (16, words))
    own = lax.broadcasted_iota(jnp.int32, (HI, GROUP, LO * GROUP), 2) % GROUP == lax.broadcasted_iota(
        jnp.int32, (HI, GROUP, LO * GROUP), 1
    )

    def pairs(x):
        return jnp.concatenate([x, x - 1], axis=0).astype(jnp.float32).astype(jnp.bfloat16)

    def group(g, carry):
        word = words_ref[pl.ds(pl.multiple_of(g * GROUP, GROUP), GROUP), :]
        total = jnp.zeros((TERMS * HI * GROUP, LO * GROUP), jnp.float32)
        for k in range(4):
            for c in range(words // 256):
                part = word[:, 256 * c : 256 * (c + 1)]
                high = pairs(jnp.bitwise_and(jnp.right_shift(part, 8 * k + 5), 7))
                low = pairs(jnp.bitwise_and(jnp.right_shift(part, 8 * k), 31))
                left = []
                for t in range(TERMS):
                    w = wts_ref[t, k, :, 256 * c : 256 * (c + 1)]
                    left += [jnp.where(high == 2 * p, w, jnp.bfloat16(0)) for p in range(HI // 2)]
                right = [
                    jnp.where(low == 2 * p, jnp.bfloat16(1), jnp.bfloat16(0)) for p in range(LO // 2)
                ]
                total += lax.dot_general(
                    jnp.concatenate(left, axis=0),
                    jnp.concatenate(right, axis=0),
                    (((1,), (1,)), ((), ())),
                    preferred_element_type=jnp.float32,
                )
        joint = jnp.sum(total.reshape(TERMS, HI, GROUP, LO * GROUP), axis=0)
        out_ref[g] = jnp.sum(jnp.where(own, joint, 0.0), axis=1)
        return carry

    lax.fori_loop(0, width // GROUP, group, 0)


def histogram(bins, hessian):
    words, width = bins.shape
    weights = hessian.reshape(words, 4).T
    return pl.pallas_call(
        hist_kernel,
        out_shape=jax.ShapeDtypeStruct((width // GROUP, HI, LO * GROUP), jnp.float32),
        scratch_shapes=[
            pltpu.VMEM((width, words), jnp.int32),
            pltpu.VMEM((TERMS, 4, 16, words), jnp.bfloat16),
        ],
        name="histogram",
    )(bins, weights)


def cuts_kernel(a_ref, b_ref, thr_ref, out_ref):
    lanes = LO * GROUP
    n_q = thr_ref.shape[1]
    hist = a_ref[...] + b_ref[...]
    src = lax.broadcasted_iota(jnp.int32, (lanes, lanes), 0)
    dst = lax.broadcasted_iota(jnp.int32, (lanes, lanes), 1)
    same = src % GROUP == dst % GROUP
    earlier = jnp.where(same & (src < dst), 1.0, 0.0)
    row = jnp.where(same, 1.0, 0.0)
    dot = lambda x, y: jnp.dot(x, y, precision=lax.Precision.HIGHEST, preferred_element_type=jnp.float32)
    before = dot(hist, earlier)
    sums = dot(hist, row)
    offset = jnp.zeros((1, lanes), jnp.float32)
    offsets = []
    for i in range(HI):
        offsets.append(offset)
        offset = offset + sums[i : i + 1, :]
    before = before + jnp.concatenate(offsets, axis=0)
    scale = 1.0 / (hist + 1.0)
    thr = jnp.broadcast_to(thr_ref[...], (n_q, n_q)).T
    halves = []
    for j in range(lanes // n_q):
        at = slice(n_q * j, n_q * (j + 1))
        target = thr * offset[:, at]
        acc = jnp.zeros((n_q, n_q), jnp.float32)
        for i in range(HI):
            acc += jnp.clip((target - before[i : i + 1, at]) * scale[i : i + 1, at], 0.0, 1.0)
        halves.append(acc)
    acc = halves[0] + halves[1]
    pick = jnp.where(
        lax.broadcasted_iota(jnp.int32, (GROUP, n_q), 1) % GROUP
        == lax.broadcasted_iota(jnp.int32, (GROUP, n_q), 0),
        1.0,
        0.0,
    )
    cuts = lax.dot_general(
        pick,
        acc,
        (((1,), (1,)), ((), ())),
        precision=lax.Precision.HIGHEST,
        preferred_element_type=jnp.float32,
    )
    out_ref[...] = jnp.broadcast_to(cuts[None], out_ref.shape)


def cut_positions(a, b, thresholds, copies):
    n_q = thresholds.shape[0]
    return pl.pallas_call(
        cuts_kernel,
        out_shape=jax.ShapeDtypeStruct((copies, GROUP, n_q), jnp.float32),
        name="cuts",
    )(a, b, thresholds.reshape(1, n_q))


def local(bins, hessian, thresholds):
    swap = [(0, 1), (1, 0)]
    pieces = histogram(bins, hessian)
    pieces = lax.all_to_all(pieces, ("x", "y"), 0, 0, tiled=True)
    part = jnp.sum(pieces, axis=0)
    part = part + lax.ppermute(part, "core", swap)
    other = lax.ppermute(part, "far", swap)
    copies = cut_positions(part, other, thresholds, pieces.shape[0])
    cuts = lax.all_to_all(copies, ("x", "y"), 0, 0, tiled=True)
    return cuts.reshape(bins.shape[1], thresholds.shape[0])


def solution(mesh):
    feat = mesh.shape["feat"]
    axes = ("x", "far", "y", "core")
    grid = Mesh(mesh.devices.reshape(4, 2, 4, 2, feat), axes + ("feat",))
    in_specs = (P(axes, "feat"), P(axes), P())
    out_specs = P("feat", None)
    return jax.shard_map(local, mesh=grid, in_specs=in_specs, out_specs=out_specs, check_vma=False)
```

```python
import jax
import jax.numpy as jnp
from jax import lax
from jax.experimental import pallas as pl
from jax.experimental.pallas import tpu as pltpu
from jax.sharding import Mesh
from jax.sharding import PartitionSpec as P

BINS = 256
HI = 8
LO = 32
GROUP = 8
PIECE = 4
TERMS = 2
LANES = 128
UNROLL = 16


def iota(shape, dim):
    return lax.broadcasted_iota(jnp.int32, shape, dim)


def hist_kernel(
    bins_hbm, hess_hbm, thr_hbm, out_ref, thr_ref, bins_ref, hess_ref, words_ref, wide_ref, wts_ref, sems
):
    words, width = bins_ref.shape
    blocks = words // LANES
    hess_copy = pltpu.make_async_copy(hess_hbm, hess_ref, sems.at[blocks])
    hess_copy.start()
    copies = []
    for i in range(blocks):
        at = pl.ds(LANES * i, LANES)
        copies.append(pltpu.make_async_copy(bins_hbm.at[at, :], bins_ref.at[at, :], sems.at[i]))
        copies[-1].start()
    thr_copy = pltpu.make_async_copy(thr_hbm, thr_ref, sems.at[blocks + 1])
    thr_copy.start()

    hess_copy.wait()
    lane = iota((blocks, LANES), 1)
    rows = [hess_ref[pl.ds(j, blocks, stride=4), :] for j in range(4)]
    for k in range(4):
        index = 4 * (lane % 32) + k
        weight = jnp.zeros((blocks, LANES), jnp.float32)
        for j in range(4):
            weight = jnp.where(lane // 32 == j, jnp.take_along_axis(rows[j], index, axis=1), weight)
        for t in range(TERMS):
            part = weight.astype(jnp.bfloat16).astype(jnp.float32)
            weight = weight - part
            for i in range(blocks):
                wts_ref[t, k, :, LANES * i : LANES * (i + 1)] = jnp.broadcast_to(
                    part[i : i + 1, :], (16, LANES)
                ).astype(jnp.bfloat16)

    for i in range(blocks):
        copies[i].wait()
        at = slice(LANES * i, LANES * (i + 1))
        turned = bins_ref[at, :].T
        words_ref[:, at] = turned
        for p in range(width // PIECE):
            four = turned[PIECE * p : PIECE * (p + 1), :]
            wide_ref[2 * PIECE * p : 2 * PIECE * (p + 1), at] = jnp.concatenate([four, four], axis=0)

    own = iota((HI, GROUP, LANES), 2) % PIECE == iota((HI, GROUP, LANES), 1) % PIECE
    first = iota((HI, GROUP, LANES), 1) < PIECE
    step16 = iota((16, LANES), 0)
    one = jnp.bfloat16(1)
    zero = jnp.bfloat16(0)

    def halves(x):
        x = jnp.concatenate([x, x], axis=0)
        return x.astype(jnp.int16), jnp.right_shift(x, 16).astype(jnp.int16)

    def group(g, carry):
        total = jnp.zeros((TERMS * HI * GROUP, 2 * LANES), jnp.float32)
        for c in range(words // 256):
            at = slice(256 * c, 256 * (c + 1))
            high = halves(words_ref[pl.ds(pl.multiple_of(g * GROUP, GROUP), GROUP), at])
            low = [
                halves(wide_ref[pl.ds(pl.multiple_of((2 * g + s) * GROUP, GROUP), GROUP), at]) for s in range(2)
            ]
            for k in range(4):
                shift = 8 * (k % 2)
                top = jnp.bitwise_and(high[k // 2], jnp.int16(int_of(224 << shift)))
                ends = [jnp.bitwise_and(low[s][k // 2], jnp.int16(31 << shift)) for s in range(2)]
                left = []
                hits = [
                    top == jnp.tile(shifted(2 * p + step16 // 8, shift + 5), (1, 2)) for p in range(HI // 2)
                ]
                for t in range(TERMS):
                    w = wts_ref[t, k, :, at]
                    left += [jnp.where(hit, w, zero) for hit in hits]
                right = [
                    jnp.where(ends[s] == jnp.tile(shifted(4 * p + step16 // 4, shift), (1, 2)), one, zero)
                    for s in range(2)
                    for p in range(LO // 4)
                ]
                total += lax.dot_general(
                    jnp.concatenate(left, axis=0),
                    jnp.concatenate(right, axis=0).astype(jnp.float8_e4m3fn),
                    (((1,), (1,)), ((), ())),
                    preferred_element_type=jnp.float32,
                )
        joint = jnp.sum(total.reshape(TERMS, HI, GROUP, 2 * LANES), axis=0)
        for s in range(2):
            keep = own & (first if s == 0 else ~first)
            out_ref[2 * g + s] = jnp.sum(jnp.where(keep, joint[:, :, LANES * s : LANES * (s + 1)], 0.0), axis=1)
        return carry

    lax.fori_loop(0, width // GROUP, group, 0, unroll=UNROLL)
    thr_copy.wait()


def int_of(x):
    return x - 65536 if x >= 32768 else x


def shifted(x, by):
    return jnp.left_shift(x, by).astype(jnp.int16)


def histogram(bins, hessian, thresholds):
    words, width = bins.shape
    n_q = thresholds.shape[0]
    hbm = pl.BlockSpec(memory_space=pl.ANY)
    return pl.pallas_call(
        hist_kernel,
        out_shape=(
            pltpu.VMEM((width // PIECE, HI, LO * PIECE), jnp.float32),
            pltpu.VMEM((1, n_q), jnp.float32),
        ),
        in_specs=[hbm, hbm, hbm],
        out_specs=(pl.BlockSpec(memory_space=pltpu.VMEM),) * 2,
        scratch_shapes=[
            pltpu.VMEM((words, width), jnp.int32),
            pltpu.VMEM((hessian.shape[0] // LANES, LANES), jnp.float32),
            pltpu.VMEM((width, words), jnp.int32),
            pltpu.VMEM((2 * width, words), jnp.int32),
            pltpu.VMEM((TERMS, 4, 16, words), jnp.bfloat16),
            pltpu.SemaphoreType.DMA((words // LANES + 2,)),
        ],
        name="histogram",
    )(bins, hessian.reshape(-1, LANES), thresholds.reshape(1, n_q))


def terms_of(x):
    parts = []
    for _ in range(2):
        parts.append(x.astype(jnp.bfloat16).astype(jnp.float32))
        x = x - parts[-1]
    return parts + [x]


def cuts_kernel(a_ref, b_ref, thr_ref, out_ref):
    hist = a_ref[...] + b_ref[...]
    src = iota((LANES, LANES), 0)
    dst = iota((LANES, LANES), 1)
    same = src % PIECE == dst % PIECE
    ones = jnp.concatenate([jnp.where(same & (src < dst), 1.0, 0.0), jnp.where(same, 1.0, 0.0)], axis=1)
    sums = jnp.dot(
        jnp.concatenate(terms_of(hist), axis=0).astype(jnp.bfloat16),
        ones.astype(jnp.bfloat16),
        preferred_element_type=jnp.float32,
    )
    sums = sums[:HI] + sums[HI : 2 * HI] + sums[2 * HI :]
    offset = jnp.zeros((1, LANES), jnp.float32)
    offsets = []
    for i in range(HI):
        offsets.append(offset)
        offset = offset + sums[i : i + 1, LANES:]
    before = sums[:, :LANES] + jnp.concatenate(offsets, axis=0)
    scale = 1.0 / (hist + 1.0)
    target = jnp.broadcast_to(thr_ref[...], (LANES, LANES)).T * offset
    acc = jnp.zeros(target.shape, jnp.float32)
    for i in range(HI):
        acc += jnp.clip((target - before[i : i + 1]) * scale[i : i + 1], 0.0, 1.0)
    n_q = acc.shape[0]
    pick = jnp.where(iota((16, LANES), 1) % PIECE == iota((16, LANES), 0), 1.0, 0.0)
    cuts = lax.dot_general(
        pick.astype(jnp.bfloat16),
        jnp.concatenate(terms_of(acc), axis=0).astype(jnp.bfloat16),
        (((1,), (1,)), ((), ())),
        preferred_element_type=jnp.float32,
    )
    cuts = cuts[:PIECE, :n_q] + cuts[:PIECE, n_q : 2 * n_q] + cuts[:PIECE, 2 * n_q :]
    out_ref[...] = jnp.broadcast_to(cuts[None], out_ref.shape)


def cut_positions(a, b, thr, copies):
    return pl.pallas_call(
        cuts_kernel,
        out_shape=pltpu.VMEM((copies, PIECE, thr.shape[1]), jnp.float32),
        in_specs=[pl.BlockSpec(memory_space=pltpu.VMEM)] * 3,
        out_specs=pl.BlockSpec(memory_space=pltpu.VMEM),
        name="cuts",
    )(*(pltpu.with_memory_space_constraint(x, pltpu.VMEM) for x in (a, b, thr)))


def local(bins, hessian, thresholds):
    near = ("x", "y", "core")
    pieces, thr = histogram(bins, hessian, thresholds)
    pieces = lax.all_to_all(pieces, near, 0, 0, tiled=True)
    part = jnp.sum(pieces, axis=0)
    other = lax.ppermute(part, "far", [(0, 1), (1, 0)])
    copies = cut_positions(part, other, thr, pieces.shape[0])
    cuts = lax.all_to_all(copies, near, 0, 0, tiled=True)
    return cuts.reshape(bins.shape[1], thresholds.shape[0])


def solution(mesh):
    feat = mesh.shape["feat"]
    axes = ("x", "far", "y", "core")
    grid = Mesh(mesh.devices.reshape(4, 2, 4, 2, feat), axes + ("feat",))
    in_specs = (P(axes, "feat"), P(axes), P())
    out_specs = P("feat", None)
    return jax.shard_map(local, mesh=grid, in_specs=in_specs, out_specs=out_specs, check_vma=False)
```

```python
import jax
import jax.numpy as jnp
from jax import lax
from jax.experimental import pallas as pl
from jax.experimental.pallas import tpu as pltpu
from jax.sharding import Mesh
from jax.sharding import PartitionSpec as P

BINS = 256
HI = 8
LO = 32
GROUP = 8
PIECE = 4
TERMS = 2
LANES = 128
UNROLL = 16


def iota(shape, dim):
    return lax.broadcasted_iota(jnp.int32, shape, dim)


def hist_kernel(
    bins_hbm, hess_hbm, thr_hbm, out_ref, thr_ref, bins_ref, hess_ref, words_ref, wide_ref, wts_ref, sems
):
    words, width = bins_ref.shape
    blocks = words // LANES
    copies = [
        pltpu.make_async_copy(hess_hbm, hess_ref, sems.at[0]),
        pltpu.make_async_copy(bins_hbm, bins_ref, sems.at[1]),
        pltpu.make_async_copy(thr_hbm, thr_ref, sems.at[2]),
    ]
    for copy in copies:
        copy.start()
    for copy in copies:
        copy.wait()

    for i in range(blocks):
        at = slice(LANES * i, LANES * (i + 1))
        turned = bins_ref[at, :].T
        words_ref[:, at] = turned
        for p in range(width // PIECE):
            four = turned[PIECE * p : PIECE * (p + 1), :]
            wide_ref[2 * PIECE * p : 2 * PIECE * (p + 1), at] = jnp.concatenate([four, four], axis=0)

    lane = iota((blocks, LANES), 1)
    rows = [hess_ref[pl.ds(j, blocks, stride=4), :] for j in range(4)]
    for k in range(4):
        index = 4 * (lane % 32) + k
        weight = jnp.zeros((blocks, LANES), jnp.float32)
        for j in range(4):
            weight = jnp.where(lane // 32 == j, jnp.take_along_axis(rows[j], index, axis=1), weight)
        for t in range(TERMS):
            part = weight.astype(jnp.bfloat16).astype(jnp.float32)
            weight = weight - part
            for i in range(blocks):
                wts_ref[t, k, :, LANES * i : LANES * (i + 1)] = jnp.broadcast_to(
                    part[i : i + 1, :], (16, LANES)
                ).astype(jnp.bfloat16)

    own = iota((HI, GROUP, LANES), 2) % PIECE == iota((HI, GROUP, LANES), 1) % PIECE
    first = iota((HI, GROUP, LANES), 1) < PIECE
    step16 = iota((16, LANES), 0)
    one = jnp.bfloat16(1)
    zero = jnp.bfloat16(0)

    def halves(x):
        x = jnp.concatenate([x, x], axis=0)
        return x.astype(jnp.int16), jnp.right_shift(x, 16).astype(jnp.int16)

    def group(g, carry):
        total = jnp.zeros((TERMS * HI * GROUP, 2 * LANES), jnp.float32)
        for c in range(words // 256):
            at = slice(256 * c, 256 * (c + 1))
            high = halves(words_ref[pl.ds(pl.multiple_of(g * GROUP, GROUP), GROUP), at])
            low = [
                halves(wide_ref[pl.ds(pl.multiple_of((2 * g + s) * GROUP, GROUP), GROUP), at]) for s in range(2)
            ]
            for k in range(4):
                shift = 8 * (k % 2)
                top = jnp.bitwise_and(high[k // 2], jnp.int16(int_of(224 << shift)))
                ends = [jnp.bitwise_and(low[s][k // 2], jnp.int16(31 << shift)) for s in range(2)]
                left = []
                hits = [
                    top == jnp.tile(shifted(2 * p + step16 // 8, shift + 5), (1, 2)) for p in range(HI // 2)
                ]
                for t in range(TERMS):
                    w = wts_ref[t, k, :, at]
                    left += [jnp.where(hit, w, zero) for hit in hits]
                right = [
                    jnp.where(ends[s] == jnp.tile(shifted(4 * p + step16 // 4, shift), (1, 2)), one, zero)
                    for s in range(2)
                    for p in range(LO // 4)
                ]
                total += lax.dot_general(
                    jnp.concatenate(left, axis=0),
                    jnp.concatenate(right, axis=0).astype(jnp.float8_e4m3fn),
                    (((1,), (1,)), ((), ())),
                    preferred_element_type=jnp.float32,
                )
        joint = jnp.sum(total.reshape(TERMS, HI, GROUP, 2 * LANES), axis=0)
        for s in range(2):
            keep = own & (first if s == 0 else ~first)
            out_ref[2 * g + s] = jnp.sum(jnp.where(keep, joint[:, :, LANES * s : LANES * (s + 1)], 0.0), axis=1)
        return carry

    lax.fori_loop(0, width // GROUP, group, 0, unroll=UNROLL)


def int_of(x):
    return x - 65536 if x >= 32768 else x


def shifted(x, by):
    return jnp.left_shift(x, by).astype(jnp.int16)


def histogram(bins, hessian, thresholds):
    words, width = bins.shape
    n_q = thresholds.shape[0]
    hbm = pl.BlockSpec(memory_space=pl.ANY)
    return pl.pallas_call(
        hist_kernel,
        out_shape=(
            pltpu.VMEM((width // PIECE, HI, LO * PIECE), jnp.float32),
            pltpu.VMEM((1, n_q), jnp.float32),
        ),
        in_specs=[hbm, hbm, hbm],
        out_specs=(pl.BlockSpec(memory_space=pltpu.VMEM),) * 2,
        scratch_shapes=[
            pltpu.VMEM((words, width), jnp.int32),
            pltpu.VMEM((hessian.shape[0] // LANES, LANES), jnp.float32),
            pltpu.VMEM((width, words), jnp.int32),
            pltpu.VMEM((2 * width, words), jnp.int32),
            pltpu.VMEM((TERMS, 4, 16, words), jnp.bfloat16),
            pltpu.SemaphoreType.DMA((3,)),
        ],
        name="histogram",
    )(bins, hessian.reshape(-1, LANES), thresholds.reshape(1, n_q))


def terms_of(x):
    parts = []
    for _ in range(2):
        parts.append(x.astype(jnp.bfloat16).astype(jnp.float32))
        x = x - parts[-1]
    return parts + [x]


def cuts_kernel(a_ref, b_ref, thr_ref, out_ref):
    hist = a_ref[...] + b_ref[...]
    src = iota((LANES, LANES), 0)
    dst = iota((LANES, LANES), 1)
    same = src % PIECE == dst % PIECE
    ones = jnp.concatenate([jnp.where(same & (src < dst), 1.0, 0.0), jnp.where(same, 1.0, 0.0)], axis=1)
    sums = jnp.dot(
        jnp.concatenate(terms_of(hist), axis=0).astype(jnp.bfloat16),
        ones.astype(jnp.bfloat16),
        preferred_element_type=jnp.float32,
    )
    sums = sums[:HI] + sums[HI : 2 * HI] + sums[2 * HI :]
    offset = jnp.zeros((1, LANES), jnp.float32)
    offsets = []
    for i in range(HI):
        offsets.append(offset)
        offset = offset + sums[i : i + 1, LANES:]
    before = sums[:, :LANES] + jnp.concatenate(offsets, axis=0)
    scale = 1.0 / (hist + 1.0)
    target = jnp.broadcast_to(thr_ref[...], (LANES, LANES)).T * offset
    acc = jnp.zeros(target.shape, jnp.float32)
    for i in range(HI):
        acc += jnp.clip((target - before[i : i + 1]) * scale[i : i + 1], 0.0, 1.0)
    n_q = acc.shape[0]
    pick = jnp.where(iota((16, LANES), 1) % PIECE == iota((16, LANES), 0), 1.0, 0.0)
    cuts = lax.dot_general(
        pick.astype(jnp.bfloat16),
        jnp.concatenate(terms_of(acc), axis=0).astype(jnp.bfloat16),
        (((1,), (1,)), ((), ())),
        preferred_element_type=jnp.float32,
    )
    cuts = cuts[:PIECE, :n_q] + cuts[:PIECE, n_q : 2 * n_q] + cuts[:PIECE, 2 * n_q :]
    out_ref[...] = jnp.broadcast_to(cuts[None], out_ref.shape)


def cut_positions(a, b, thr, copies):
    return pl.pallas_call(
        cuts_kernel,
        out_shape=pltpu.VMEM((copies, PIECE, thr.shape[1]), jnp.float32),
        in_specs=[pl.BlockSpec(memory_space=pltpu.VMEM)] * 3,
        out_specs=pl.BlockSpec(memory_space=pltpu.VMEM),
        name="cuts",
    )(*(pltpu.with_memory_space_constraint(x, pltpu.VMEM) for x in (a, b, thr)))


def local(bins, hessian, thresholds):
    near = ("x", "y", "core")
    pieces, thr = histogram(bins, hessian, thresholds)
    pieces = lax.all_to_all(pieces, near, 0, 0, tiled=True)
    part = jnp.sum(pieces, axis=0)
    other = lax.ppermute(part, "far", [(0, 1), (1, 0)])
    copies = cut_positions(part, other, thr, pieces.shape[0])
    cuts = lax.all_to_all(copies, near, 0, 0, tiled=True)
    return cuts.reshape(bins.shape[1], thresholds.shape[0])


def solution(mesh):
    feat = mesh.shape["feat"]
    axes = ("x", "far", "y", "core")
    grid = Mesh(mesh.devices.reshape(4, 2, 4, 2, feat), axes + ("feat",))
    in_specs = (P(axes, "feat"), P(axes), P())
    out_specs = P("feat", None)
    return jax.shard_map(local, mesh=grid, in_specs=in_specs, out_specs=out_specs, check_vma=False)
```

```python
import jax
import jax.numpy as jnp
from jax import lax
from jax.experimental import pallas as pl
from jax.experimental.pallas import tpu as pltpu
from jax.sharding import PartitionSpec as P

BINS = 256
HI = 8
LO = 32
GROUP = 8
PIECE = 4
TERMS = 2
LANES = 128
UNROLL = 16


def iota(shape, dim):
    return lax.broadcasted_iota(jnp.int32, shape, dim)


def hist_kernel(
    bins_hbm, hess_hbm, thr_hbm, out_ref, thr_ref, bins_ref, hess_ref, words_ref, wide_ref, wts_ref, sems
):
    words, width = bins_ref.shape
    blocks = words // LANES
    copies = [
        pltpu.make_async_copy(hess_hbm, hess_ref, sems.at[0]),
        pltpu.make_async_copy(bins_hbm, bins_ref, sems.at[1]),
        pltpu.make_async_copy(thr_hbm, thr_ref, sems.at[2]),
    ]
    for copy in copies:
        copy.start()
    for copy in copies:
        copy.wait()

    for i in range(blocks):
        at = slice(LANES * i, LANES * (i + 1))
        turned = bins_ref[at, :].T
        words_ref[:, at] = turned
        for p in range(width // PIECE):
            four = turned[PIECE * p : PIECE * (p + 1), :]
            wide_ref[2 * PIECE * p : 2 * PIECE * (p + 1), at] = jnp.concatenate([four, four], axis=0)

    lane = iota((blocks, LANES), 1)
    rows = [hess_ref[pl.ds(j, blocks, stride=4), :] for j in range(4)]
    for k in range(4):
        index = 4 * (lane % 32) + k
        weight = jnp.zeros((blocks, LANES), jnp.float32)
        for j in range(4):
            weight = jnp.where(lane // 32 == j, jnp.take_along_axis(rows[j], index, axis=1), weight)
        for t in range(TERMS):
            part = weight.astype(jnp.bfloat16).astype(jnp.float32)
            weight = weight - part
            for i in range(blocks):
                wts_ref[t, k, :, LANES * i : LANES * (i + 1)] = jnp.broadcast_to(
                    part[i : i + 1, :], (16, LANES)
                ).astype(jnp.bfloat16)

    own = iota((HI, GROUP, LANES), 2) % PIECE == iota((HI, GROUP, LANES), 1) % PIECE
    first = iota((HI, GROUP, LANES), 1) < PIECE
    step16 = iota((16, LANES), 0)
    one = jnp.bfloat16(1)
    zero = jnp.bfloat16(0)

    def halves(x):
        x = jnp.concatenate([x, x], axis=0)
        return x.astype(jnp.int16), jnp.right_shift(x, 16).astype(jnp.int16)

    def group(g, carry):
        total = jnp.zeros((TERMS * HI * GROUP, 2 * LANES), jnp.float32)
        for c in range(words // 256):
            at = slice(256 * c, 256 * (c + 1))
            high = halves(words_ref[pl.ds(pl.multiple_of(g * GROUP, GROUP), GROUP), at])
            low = [
                halves(wide_ref[pl.ds(pl.multiple_of((2 * g + s) * GROUP, GROUP), GROUP), at]) for s in range(2)
            ]
            for k in range(4):
                shift = 8 * (k % 2)
                top = jnp.bitwise_and(high[k // 2], jnp.int16(int_of(224 << shift)))
                ends = [jnp.bitwise_and(low[s][k // 2], jnp.int16(31 << shift)) for s in range(2)]
                left = []
                hits = [
                    top == jnp.tile(shifted(2 * p + step16 // 8, shift + 5), (1, 2)) for p in range(HI // 2)
                ]
                for t in range(TERMS):
                    w = wts_ref[t, k, :, at]
                    left += [jnp.where(hit, w, zero) for hit in hits]
                right = [
                    jnp.where(ends[s] == jnp.tile(shifted(4 * p + step16 // 4, shift), (1, 2)), one, zero)
                    for s in range(2)
                    for p in range(LO // 4)
                ]
                total += lax.dot_general(
                    jnp.concatenate(left, axis=0),
                    jnp.concatenate(right, axis=0).astype(jnp.float8_e4m3fn),
                    (((1,), (1,)), ((), ())),
                    preferred_element_type=jnp.float32,
                )
        joint = jnp.sum(total.reshape(TERMS, HI, GROUP, 2 * LANES), axis=0)
        for s in range(2):
            keep = own & (first if s == 0 else ~first)
            out_ref[2 * g + s] = jnp.sum(jnp.where(keep, joint[:, :, LANES * s : LANES * (s + 1)], 0.0), axis=1)
        return carry

    lax.fori_loop(0, width // GROUP, group, 0, unroll=UNROLL)


def int_of(x):
    return x - 65536 if x >= 32768 else x


def shifted(x, by):
    return jnp.left_shift(x, by).astype(jnp.int16)


def histogram(bins, hessian, thresholds):
    words, width = bins.shape
    n_q = thresholds.shape[0]
    hbm = pl.BlockSpec(memory_space=pl.ANY)
    return pl.pallas_call(
        hist_kernel,
        out_shape=(
            pltpu.VMEM((width // PIECE, HI, LO * PIECE), jnp.float32),
            pltpu.VMEM((1, n_q), jnp.float32),
        ),
        in_specs=[hbm, hbm, hbm],
        out_specs=(pl.BlockSpec(memory_space=pltpu.VMEM),) * 2,
        scratch_shapes=[
            pltpu.VMEM((words, width), jnp.int32),
            pltpu.VMEM((hessian.shape[0] // LANES, LANES), jnp.float32),
            pltpu.VMEM((width, words), jnp.int32),
            pltpu.VMEM((2 * width, words), jnp.int32),
            pltpu.VMEM((TERMS, 4, 16, words), jnp.bfloat16),
            pltpu.SemaphoreType.DMA((3,)),
        ],
        name="histogram",
    )(bins, hessian.reshape(-1, LANES), thresholds.reshape(1, n_q))


def terms_of(x):
    parts = []
    for _ in range(2):
        parts.append(x.astype(jnp.bfloat16).astype(jnp.float32))
        x = x - parts[-1]
    return parts + [x]


def cuts_kernel(a_ref, b_ref, thr_ref, out_ref):
    hist = a_ref[...] + b_ref[...]
    src = iota((LANES, LANES), 0)
    dst = iota((LANES, LANES), 1)
    same = src % PIECE == dst % PIECE
    ones = jnp.concatenate([jnp.where(same & (src < dst), 1.0, 0.0), jnp.where(same, 1.0, 0.0)], axis=1)
    sums = jnp.dot(
        jnp.concatenate(terms_of(hist), axis=0).astype(jnp.bfloat16),
        ones.astype(jnp.bfloat16),
        preferred_element_type=jnp.float32,
    )
    sums = sums[:HI] + sums[HI : 2 * HI] + sums[2 * HI :]
    offset = jnp.zeros((1, LANES), jnp.float32)
    offsets = []
    for i in range(HI):
        offsets.append(offset)
        offset = offset + sums[i : i + 1, LANES:]
    before = sums[:, :LANES] + jnp.concatenate(offsets, axis=0)
    scale = 1.0 / (hist + 1.0)
    target = jnp.broadcast_to(thr_ref[...], (LANES, LANES)).T * offset
    acc = jnp.zeros(target.shape, jnp.float32)
    for i in range(HI):
        acc += jnp.clip((target - before[i : i + 1]) * scale[i : i + 1], 0.0, 1.0)
    n_q = acc.shape[0]
    pick = jnp.where(iota((16, LANES), 1) % PIECE == iota((16, LANES), 0), 1.0, 0.0)
    cuts = lax.dot_general(
        pick.astype(jnp.bfloat16),
        jnp.concatenate(terms_of(acc), axis=0).astype(jnp.bfloat16),
        (((1,), (1,)), ((), ())),
        preferred_element_type=jnp.float32,
    )
    cuts = cuts[:PIECE, :n_q] + cuts[:PIECE, n_q : 2 * n_q] + cuts[:PIECE, 2 * n_q :]
    out_ref[...] = jnp.broadcast_to(cuts[None], out_ref.shape)


def cut_positions(a, b, thr, copies):
    return pl.pallas_call(
        cuts_kernel,
        out_shape=pltpu.VMEM((copies, PIECE, thr.shape[1]), jnp.float32),
        in_specs=[pl.BlockSpec(memory_space=pltpu.VMEM)] * 3,
        out_specs=pl.BlockSpec(memory_space=pltpu.VMEM),
        name="cuts",
    )(*(pltpu.with_memory_space_constraint(x, pltpu.VMEM) for x in (a, b, thr)))


def groups_of(first):
    x0, y0, c0 = first
    return [
        [
            (((x0 + x) % 4 * 2 + far) * 4 + (y0 + y) % 4) * 2 + (c0 + c) % 2
            for x in range(4)
            for y in range(4)
            for c in range(2)
        ]
        for far in range(2)
    ]


FIRST = (2, 2, 1)


def local(bins, hessian, thresholds):
    near = groups_of(FIRST)
    swap = [(i, i ^ 8) for i in range(64)]
    pieces, thr = histogram(bins, hessian, thresholds)
    pieces = lax.all_to_all(pieces, "rows", 0, 0, axis_index_groups=near, tiled=True)
    part = jnp.sum(pieces, axis=0)
    other = lax.ppermute(part, "rows", swap)
    copies = cut_positions(part, other, thr, pieces.shape[0])
    cuts = lax.all_to_all(copies, "rows", 0, 0, axis_index_groups=near, tiled=True)
    return cuts.reshape(bins.shape[1], thresholds.shape[0])


def solution(mesh):
    in_specs = (P("rows", "feat"), P("rows"), P())
    out_specs = P("feat", None)
    return jax.shard_map(local, mesh=mesh, in_specs=in_specs, out_specs=out_specs, check_vma=False)
```

```python
import jax
import jax.numpy as jnp
from jax import lax
from jax.experimental import pallas as pl
from jax.experimental.pallas import tpu as pltpu
from jax.sharding import PartitionSpec as P

BINS = 256
HI = 8
LO = 32
GROUP = 8
PIECE = 4
TERMS = 2
LANES = 128
UNROLL = 16


def iota(shape, dim):
    return lax.broadcasted_iota(jnp.int32, shape, dim)


def hist_kernel(
    bins_hbm, hess_hbm, thr_hbm, out_ref, thr_ref, bins_ref, hess_ref, words_ref, wide_ref, wts_ref, sems
):
    words, width = bins_ref.shape
    blocks = words // LANES
    copies = [
        pltpu.make_async_copy(hess_hbm, hess_ref, sems.at[0]),
        pltpu.make_async_copy(bins_hbm, bins_ref, sems.at[1]),
        pltpu.make_async_copy(thr_hbm, thr_ref, sems.at[2]),
    ]
    for copy in copies:
        copy.start()
    for copy in copies:
        copy.wait()

    for i in range(blocks):
        at = slice(LANES * i, LANES * (i + 1))
        turned = bins_ref[at, :].T
        words_ref[:, at] = turned
        for p in range(width // PIECE):
            four = turned[PIECE * p : PIECE * (p + 1), :]
            wide_ref[2 * PIECE * p : 2 * PIECE * (p + 1), at] = jnp.concatenate([four, four], axis=0)

    lane = iota((blocks, LANES), 1)
    rows = [hess_ref[pl.ds(j, blocks, stride=4), :] for j in range(4)]
    for k in range(4):
        index = 4 * (lane % 32) + k
        weight = jnp.zeros((blocks, LANES), jnp.float32)
        for j in range(4):
            weight = jnp.where(lane // 32 == j, jnp.take_along_axis(rows[j], index, axis=1), weight)
        for t in range(TERMS):
            part = weight.astype(jnp.bfloat16).astype(jnp.float32)
            weight = weight - part
            for i in range(blocks):
                wts_ref[t, k, :, LANES * i : LANES * (i + 1)] = jnp.broadcast_to(
                    part[i : i + 1, :], (16, LANES)
                ).astype(jnp.bfloat16)

    own = iota((HI, GROUP, LANES), 2) % PIECE == iota((HI, GROUP, LANES), 1) % PIECE
    first = iota((HI, GROUP, LANES), 1) < PIECE
    step16 = iota((16, LANES), 0)
    one = jnp.bfloat16(1)
    zero = jnp.bfloat16(0)

    def halves(x):
        x = jnp.concatenate([x, x], axis=0)
        return x.astype(jnp.int16), jnp.right_shift(x, 16).astype(jnp.int16)

    def group(g, carry):
        total = jnp.zeros((TERMS * HI * GROUP, 2 * LANES), jnp.float32)
        for c in range(words // 256):
            at = slice(256 * c, 256 * (c + 1))
            high = halves(words_ref[pl.ds(pl.multiple_of(g * GROUP, GROUP), GROUP), at])
            low = [
                halves(wide_ref[pl.ds(pl.multiple_of((2 * g + s) * GROUP, GROUP), GROUP), at]) for s in range(2)
            ]
            for k in range(4):
                shift = 8 * (k % 2)
                top = jnp.bitwise_and(high[k // 2], jnp.int16(int_of(224 << shift)))
                ends = [jnp.bitwise_and(low[s][k // 2], jnp.int16(31 << shift)) for s in range(2)]
                left = []
                hits = [
                    top == jnp.tile(shifted(2 * p + step16 // 8, shift + 5), (1, 2)) for p in range(HI // 2)
                ]
                for t in range(TERMS):
                    w = wts_ref[t, k, :, at]
                    left += [jnp.where(hit, w, zero) for hit in hits]
                right = [
                    jnp.where(ends[s] == jnp.tile(shifted(4 * p + step16 // 4, shift), (1, 2)), one, zero)
                    for s in range(2)
                    for p in range(LO // 4)
                ]
                total += lax.dot_general(
                    jnp.concatenate(left, axis=0),
                    jnp.concatenate(right, axis=0).astype(jnp.float8_e4m3fn),
                    (((1,), (1,)), ((), ())),
                    preferred_element_type=jnp.float32,
                )
        joint = jnp.sum(total.reshape(TERMS, HI, GROUP, 2 * LANES), axis=0)
        for s in range(2):
            keep = own & (first if s == 0 else ~first)
            out_ref[2 * g + s] = jnp.sum(jnp.where(keep, joint[:, :, LANES * s : LANES * (s + 1)], 0.0), axis=1)
        return carry

    lax.fori_loop(0, width // GROUP, group, 0, unroll=UNROLL)


def int_of(x):
    return x - 65536 if x >= 32768 else x


def shifted(x, by):
    return jnp.left_shift(x, by).astype(jnp.int16)


def histogram(bins, hessian, thresholds):
    words, width = bins.shape
    n_q = thresholds.shape[0]
    hbm = pl.BlockSpec(memory_space=pl.ANY)
    return pl.pallas_call(
        hist_kernel,
        out_shape=(
            pltpu.VMEM((width // PIECE, HI, LO * PIECE), jnp.float32),
            pltpu.VMEM((1, n_q), jnp.float32),
        ),
        in_specs=[hbm, hbm, hbm],
        out_specs=(pl.BlockSpec(memory_space=pltpu.VMEM),) * 2,
        scratch_shapes=[
            pltpu.VMEM((words, width), jnp.int32),
            pltpu.VMEM((hessian.shape[0] // LANES, LANES), jnp.float32),
            pltpu.VMEM((width, words), jnp.int32),
            pltpu.VMEM((2 * width, words), jnp.int32),
            pltpu.VMEM((TERMS, 4, 16, words), jnp.bfloat16),
            pltpu.SemaphoreType.DMA((3,)),
        ],
        name="histogram",
    )(bins, hessian.reshape(-1, LANES), thresholds.reshape(1, n_q))


def terms_of(x):
    parts = []
    for _ in range(2):
        parts.append(x.astype(jnp.bfloat16).astype(jnp.float32))
        x = x - parts[-1]
    return parts + [x]


def cuts_kernel(a_ref, b_ref, thr_ref, out_ref):
    hist = a_ref[...] + b_ref[...]
    src = iota((LANES, LANES), 0)
    dst = iota((LANES, LANES), 1)
    same = src % PIECE == dst % PIECE
    ones = jnp.concatenate([jnp.where(same & (src < dst), 1.0, 0.0), jnp.where(same, 1.0, 0.0)], axis=1)
    sums = jnp.dot(
        jnp.concatenate(terms_of(hist), axis=0).astype(jnp.bfloat16),
        ones.astype(jnp.bfloat16),
        preferred_element_type=jnp.float32,
    )
    sums = sums[:HI] + sums[HI : 2 * HI] + sums[2 * HI :]
    offset = jnp.zeros((1, LANES), jnp.float32)
    offsets = []
    for i in range(HI):
        offsets.append(offset)
        offset = offset + sums[i : i + 1, LANES:]
    before = sums[:, :LANES] + jnp.concatenate(offsets, axis=0)
    scale = 1.0 / (hist + 1.0)
    target = jnp.broadcast_to(thr_ref[...], (LANES, LANES)).T * offset
    acc = jnp.zeros(target.shape, jnp.float32)
    for i in range(HI):
        acc += jnp.clip((target - before[i : i + 1]) * scale[i : i + 1], 0.0, 1.0)
    n_q = acc.shape[0]
    pick = jnp.where(iota((16, LANES), 1) % PIECE == iota((16, LANES), 0), 1.0, 0.0)
    cuts = lax.dot_general(
        pick.astype(jnp.bfloat16),
        jnp.concatenate(terms_of(acc), axis=0).astype(jnp.bfloat16),
        (((1,), (1,)), ((), ())),
        preferred_element_type=jnp.float32,
    )
    cuts = cuts[:PIECE, :n_q] + cuts[:PIECE, n_q : 2 * n_q] + cuts[:PIECE, 2 * n_q :]
    out_ref[...] = jnp.broadcast_to(cuts[None], out_ref.shape)


def cut_positions(a, b, thr, copies):
    return pl.pallas_call(
        cuts_kernel,
        out_shape=pltpu.VMEM((copies, PIECE, thr.shape[1]), jnp.float32),
        in_specs=[pl.BlockSpec(memory_space=pltpu.VMEM)] * 3,
        out_specs=pl.BlockSpec(memory_space=pltpu.VMEM),
        name="cuts",
    )(*(pltpu.with_memory_space_constraint(x, pltpu.VMEM) for x in (a, b, thr)))


def groups_of(first):
    x0, y0, c0 = first
    return [
        [
            (((x0 + x) % 4 * 2 + far) * 4 + (y0 + y) % 4) * 2 + (c0 + c + 1 - far) % 2
            for x in range(4)
            for y in range(4)
            for c in range(2)
        ]
        for far in range(2)
    ]


FIRST = (2, 2, 1)


def local(bins, hessian, thresholds):
    near = groups_of(FIRST)
    swap = [(i, i ^ 9) for i in range(64)]
    pieces, thr = histogram(bins, hessian, thresholds)
    pieces = lax.all_to_all(pieces, "rows", 0, 0, axis_index_groups=near, tiled=True)
    part = jnp.sum(pieces, axis=0)
    other = lax.ppermute(part, "rows", swap)
    copies = cut_positions(part, other, thr, pieces.shape[0])
    cuts = lax.all_to_all(copies, "rows", 0, 0, axis_index_groups=near, tiled=True)
    return cuts.reshape(bins.shape[1], thresholds.shape[0])


def solution(mesh):
    in_specs = (P("rows", "feat"), P("rows"), P())
    out_specs = P("feat", None)
    return jax.shard_map(local, mesh=mesh, in_specs=in_specs, out_specs=out_specs, check_vma=False)
```

```python
import jax
import jax.numpy as jnp
from jax import lax
from jax.experimental import pallas as pl
from jax.experimental.pallas import tpu as pltpu
from jax.sharding import PartitionSpec as P

BINS = 256
HI = 8
LO = 32
GROUP = 8
PIECE = 4
TERMS = 2
LANES = 128
UNROLL = 16


def iota(shape, dim):
    return lax.broadcasted_iota(jnp.int32, shape, dim)


def hist_kernel(
    bins_hbm, hess_hbm, thr_hbm, out_ref, thr_ref, bins_ref, hess_ref, words_ref, wide_ref, wts_ref, sems
):
    words, width = bins_ref.shape
    blocks = words // LANES
    copies = [
        pltpu.make_async_copy(bins_hbm, bins_ref, sems.at[0]),
        pltpu.make_async_copy(hess_hbm, hess_ref, sems.at[1]),
        pltpu.make_async_copy(thr_hbm, thr_ref, sems.at[2]),
    ]
    for copy in copies:
        copy.start()
    for copy in copies[:2]:
        copy.wait()

    for i in range(blocks):
        at = slice(LANES * i, LANES * (i + 1))
        turned = bins_ref[at, :].T
        words_ref[:, at] = turned
        for p in range(width // PIECE):
            four = turned[PIECE * p : PIECE * (p + 1), :]
            wide_ref[2 * PIECE * p : 2 * PIECE * (p + 1), at] = jnp.concatenate([four, four], axis=0)

    lane = iota((blocks, LANES), 1)
    rows = [hess_ref[pl.ds(j, blocks, stride=4), :] for j in range(4)]
    for k in range(4):
        index = 4 * (lane % 32) + k
        weight = jnp.zeros((blocks, LANES), jnp.float32)
        for j in range(4):
            weight = jnp.where(lane // 32 == j, jnp.take_along_axis(rows[j], index, axis=1), weight)
        for t in range(TERMS):
            part = weight.astype(jnp.bfloat16).astype(jnp.float32)
            weight = weight - part
            for i in range(blocks):
                wts_ref[t, k, :, LANES * i : LANES * (i + 1)] = jnp.broadcast_to(
                    part[i : i + 1, :], (16, LANES)
                ).astype(jnp.bfloat16)

    own = iota((HI, GROUP, LANES), 2) % PIECE == iota((HI, GROUP, LANES), 1) % PIECE
    first = iota((HI, GROUP, LANES), 1) < PIECE
    step16 = iota((16, LANES), 0)
    one = jnp.bfloat16(1)
    zero = jnp.bfloat16(0)

    def halves(x):
        x = jnp.concatenate([x, x], axis=0)
        return x.astype(jnp.int16), jnp.right_shift(x, 16).astype(jnp.int16)

    def group(g, carry):
        total = jnp.zeros((TERMS * HI * GROUP, 2 * LANES), jnp.float32)
        for c in range(words // 256):
            at = slice(256 * c, 256 * (c + 1))
            high = halves(words_ref[pl.ds(pl.multiple_of(g * GROUP, GROUP), GROUP), at])
            low = [
                halves(wide_ref[pl.ds(pl.multiple_of((2 * g + s) * GROUP, GROUP), GROUP), at]) for s in range(2)
            ]
            for k in range(4):
                shift = 8 * (k % 2)
                top = jnp.bitwise_and(high[k // 2], jnp.int16(int_of(224 << shift)))
                ends = [jnp.bitwise_and(low[s][k // 2], jnp.int16(31 << shift)) for s in range(2)]
                left = []
                hits = [
                    top == jnp.tile(shifted(2 * p + step16 // 8, shift + 5), (1, 2)) for p in range(HI // 2)
                ]
                for t in range(TERMS):
                    w = wts_ref[t, k, :, at]
                    left += [jnp.where(hit, w, zero) for hit in hits]
                right = [
                    jnp.where(ends[s] == jnp.tile(shifted(4 * p + step16 // 4, shift), (1, 2)), one, zero)
                    for s in range(2)
                    for p in range(LO // 4)
                ]
                total += lax.dot_general(
                    jnp.concatenate(left, axis=0),
                    jnp.concatenate(right, axis=0).astype(jnp.float8_e4m3fn),
                    (((1,), (1,)), ((), ())),
                    preferred_element_type=jnp.float32,
                )
        joint = jnp.sum(total.reshape(TERMS, HI, GROUP, 2 * LANES), axis=0)
        for s in range(2):
            keep = own & (first if s == 0 else ~first)
            out_ref[2 * g + s] = jnp.sum(jnp.where(keep, joint[:, :, LANES * s : LANES * (s + 1)], 0.0), axis=1)
        return carry

    lax.fori_loop(0, width // GROUP, group, 0, unroll=UNROLL)
    copies[2].wait()


def int_of(x):
    return x - 65536 if x >= 32768 else x


def shifted(x, by):
    return jnp.left_shift(x, by).astype(jnp.int16)


def histogram(bins, hessian, thresholds):
    words, width = bins.shape
    n_q = thresholds.shape[0]
    hbm = pl.BlockSpec(memory_space=pl.ANY)
    return pl.pallas_call(
        hist_kernel,
        out_shape=(
            pltpu.VMEM((width // PIECE, HI, LO * PIECE), jnp.float32),
            pltpu.VMEM((1, n_q), jnp.float32),
        ),
        in_specs=[hbm, hbm, hbm],
        out_specs=(pl.BlockSpec(memory_space=pltpu.VMEM),) * 2,
        scratch_shapes=[
            pltpu.VMEM((words, width), jnp.int32),
            pltpu.VMEM((hessian.shape[0] // LANES, LANES), jnp.float32),
            pltpu.VMEM((width, words), jnp.int32),
            pltpu.VMEM((2 * width, words), jnp.int32),
            pltpu.VMEM((TERMS, 4, 16, words), jnp.bfloat16),
            pltpu.SemaphoreType.DMA((3,)),
        ],
        name="histogram",
    )(bins, hessian.reshape(-1, LANES), thresholds.reshape(1, n_q))


def terms_of(x):
    parts = []
    for _ in range(2):
        parts.append(x.astype(jnp.bfloat16).astype(jnp.float32))
        x = x - parts[-1]
    return parts + [x]


def cuts_kernel(a_ref, b_ref, thr_ref, out_ref):
    hist = a_ref[...] + b_ref[...]
    src = iota((LANES, LANES), 0)
    dst = iota((LANES, LANES), 1)
    same = src % PIECE == dst % PIECE
    ones = jnp.concatenate([jnp.where(same & (src < dst), 1.0, 0.0), jnp.where(same, 1.0, 0.0)], axis=1)
    sums = jnp.dot(
        jnp.concatenate(terms_of(hist), axis=0).astype(jnp.bfloat16),
        ones.astype(jnp.bfloat16),
        preferred_element_type=jnp.float32,
    )
    sums = sums[:HI] + sums[HI : 2 * HI] + sums[2 * HI :]
    offset = jnp.zeros((1, LANES), jnp.float32)
    offsets = []
    for i in range(HI):
        offsets.append(offset)
        offset = offset + sums[i : i + 1, LANES:]
    before = sums[:, :LANES] + jnp.concatenate(offsets, axis=0)
    scale = 1.0 / (hist + 1.0)
    target = jnp.broadcast_to(thr_ref[...], (LANES, LANES)).T * offset
    acc = jnp.zeros(target.shape, jnp.float32)
    for i in range(HI):
        acc += jnp.clip((target - before[i : i + 1]) * scale[i : i + 1], 0.0, 1.0)
    n_q = acc.shape[0]
    pick = jnp.where(iota((16, LANES), 1) % PIECE == iota((16, LANES), 0), 1.0, 0.0)
    cuts = lax.dot_general(
        pick.astype(jnp.bfloat16),
        jnp.concatenate(terms_of(acc), axis=0).astype(jnp.bfloat16),
        (((1,), (1,)), ((), ())),
        preferred_element_type=jnp.float32,
    )
    cuts = cuts[:PIECE, :n_q] + cuts[:PIECE, n_q : 2 * n_q] + cuts[:PIECE, 2 * n_q :]
    out_ref[...] = jnp.broadcast_to(cuts[None], out_ref.shape)


def cut_positions(a, b, thr, copies):
    return pl.pallas_call(
        cuts_kernel,
        out_shape=pltpu.VMEM((copies, PIECE, thr.shape[1]), jnp.float32),
        in_specs=[pl.BlockSpec(memory_space=pltpu.VMEM)] * 3,
        out_specs=pl.BlockSpec(memory_space=pltpu.VMEM),
        name="cuts",
    )(*(pltpu.with_memory_space_constraint(x, pltpu.VMEM) for x in (a, b, thr)))


def groups_of(first):
    x0, y0, c0 = first
    return [
        [
            (((x0 + x) % 4 * 2 + far) * 4 + (y0 + y) % 4) * 2 + (c0 + c + 1 - far) % 2
            for x in range(4)
            for y in range(4)
            for c in range(2)
        ]
        for far in range(2)
    ]


FIRST = (2, 2, 1)


def local(bins, hessian, thresholds):
    near = groups_of(FIRST)
    swap = [(i, i ^ 9) for i in range(64)]
    pieces, thr = histogram(bins, hessian, thresholds)
    pieces = lax.all_to_all(pieces, "rows", 0, 0, axis_index_groups=near, tiled=True)
    part = jnp.sum(pieces, axis=0)
    other = lax.ppermute(part, "rows", swap)
    copies = cut_positions(part, other, thr, pieces.shape[0])
    cuts = lax.all_to_all(copies, "rows", 0, 0, axis_index_groups=near, tiled=True)
    return cuts.reshape(bins.shape[1], thresholds.shape[0])


def solution(mesh):
    in_specs = (P("rows", "feat"), P("rows"), P())
    out_specs = P("feat", None)
    return jax.shard_map(local, mesh=mesh, in_specs=in_specs, out_specs=out_specs, check_vma=False)
```
